32 devices in a mesh: ctx: 16 (over z, y, x), head: 2 (over core).
Axes of the slice: x: 2, y: 2, z: 4, core: 2. Of those that a mesh axis runs over, the one named last changes fastest.
Arguments:
- compressed: bfloat16 [3072, 576], P('ctx'), may hold values from -40 to 40
- query: bfloat16 [3072, 128, 192], P('ctx', 'head'), may hold values from -100 to 100
- d_output: bfloat16 [3072, 128, 128], P('ctx', 'head'), may hold values from -6 to 6
- w_uk: bfloat16 [512, 128, 128], P(None, 'head'), may hold values from -0.25 to 0.25
- w_uv: bfloat16 [512, 128, 128], P(None, 'head'), may hold values from -0.25 to 0.25
Outputs:
- d_query: float32 [3072, 128, 192], P('ctx', 'head')
- d_compressed: float32 [3072, 576], P(('ctx', 'head'))
- d_w_uk: float32 [512, 128, 128], P('ctx', 'head')
- d_w_uv: float32 [512, 128, 128], P('ctx', 'head')
The draws below stay inside these ranges and needn't reach their ends.
All inputs are finite; a program needn't handle non-finite values.
Results may differ from the reference program's by a relative error of at most 0.012.
Values may be sent and summed in bfloat16 or wider, within the bound.
No kernel may reach another device: no remote copies, remote signals or barrier semaphores. Data moves between devices by JAX's collectives and lax.ppermute only.
A program may use at most 256 MiB of HBM per device.

```python
import math
import jax
import jax.numpy as jnp
from jax import lax

HEADS = 128
NOPE_DIM = 128
ROPE_DIM = 64
VALUE_DIM = 128
LATENT = 512
TOK_DEV = 192
GROUP = 4
TOKENS = 3072


def shared_draw(key):
    folded = jax.random.fold_in(key, 17)
    subkeys = jax.random.split(folded, 6)
    latent_part = jnp.clip(jax.random.normal(subkeys[1], (TOKENS, LATENT), jnp.float32), -6.0, 6.0)
    rope_part = jnp.clip(jax.random.normal(subkeys[3], (TOKENS, ROPE_DIM), jnp.float32), -6.0, 6.0)
    query_nope = jnp.clip(jax.random.normal(subkeys[4], (TOKENS, HEADS, NOPE_DIM), jnp.float32), -6.0, 6.0)
    query_rope = jnp.clip(jax.random.normal(subkeys[5], (TOKENS, HEADS, ROPE_DIM), jnp.float32), -6.0, 6.0)
    compressed_rows = jnp.concatenate([latent_part, rope_part], axis=1)
    query_rows = jnp.concatenate([query_nope, query_rope], axis=2)
    return (compressed_rows, query_rows)


def draw_compressed(key, part):
    return shared_draw(key)[0].astype(jnp.bfloat16)


def draw_query(key, part):
    return shared_draw(key)[1].astype(jnp.bfloat16)


def levels(rng, shape, shards, smallest, high):
    level = 1.0
    for axis_at, blocks in shards:
        heights = jax.random.uniform(jax.random.fold_in(jax.random.fold_in(rng, 6), axis_at), (blocks,), jnp.float32, smallest / len(shards), high / len(shards))
        level = level * jnp.repeat(jnp.exp(heights), shape[axis_at] // blocks).reshape((-1,) + (1,) * (len(shape) - 1 - axis_at))
    return level


def normal_values(stream_key, dims, scale, most, cuts=(), kind=jnp.bfloat16):
    result = jax.random.normal(stream_key, dims, jnp.float32) * scale
    if len(cuts) > 0:
        result = levels(stream_key, dims, cuts, -0.22, 0.18) * result
    return jnp.clip(result, min=-most, max=most).astype(kind)


def setup_inputs(seed: int = 0) -> dict:
    key_list = jax.random.split(jax.random.key(seed), 6)
    compressed = draw_compressed(jax.random.fold_in(key_list[5], 71), 0)
    query = draw_query(jax.random.fold_in(key_list[5], 71), 0)
    d_output = normal_values(key_list[2], (TOKENS, HEADS, VALUE_DIM), 1.0, 6.0, ((0, 16), (1, 2)))
    w_uk = normal_values(key_list[3], (LATENT, HEADS, NOPE_DIM), LATENT ** -0.5, 0.25, ((1, 2),))
    w_uv = normal_values(key_list[4], (LATENT, HEADS, VALUE_DIM), LATENT ** -0.5, 0.25, ((1, 2),))
    return {"compressed": compressed, "query": query, "d_output": d_output, "w_uk": w_uk, "w_uv": w_uv}


def expand_latent(latent, weight):
    return jnp.einsum('jc,chd->jhd', latent.astype(jnp.float32), weight.astype(jnp.float32)).astype(jnp.bfloat16)

def reference(compressed, query, d_output, w_uk, w_uv):
    span_rows = GROUP * TOK_DEV
    nope_width = w_uk.shape[2]
    score_scale = 1.0 / math.sqrt(query.shape[2])
    uk_wide = w_uk.astype(jnp.float32)
    uv_wide = w_uv.astype(jnp.float32)

    def one_sequence(totals, sequence):
        grad_uk, grad_uv = totals
        first_row = (sequence * span_rows).astype(jnp.int32)
        row_block = lax.dynamic_slice_in_dim(compressed, first_row, span_rows, 0)
        latent = row_block[:, :LATENT]
        key_rope = row_block[:, LATENT:].astype(jnp.float32)
        key_nope = expand_latent(latent, w_uk).astype(jnp.float32)
        values_here = expand_latent(latent, w_uv).astype(jnp.float32)
        key_total = jnp.zeros((span_rows, HEADS, NOPE_DIM), jnp.float32)
        value_total = jnp.zeros((span_rows, HEADS, VALUE_DIM), jnp.float32)
        rope_total = jnp.zeros((span_rows, ROPE_DIM), jnp.float32)
        query_grads = []
        for slab_index in range(GROUP):
            slab_start = (first_row + slab_index * TOK_DEV).astype(jnp.int32)
            query_slab = lax.dynamic_slice_in_dim(query, slab_start, TOK_DEV, 0).astype(jnp.float32)
            output_grad = lax.dynamic_slice_in_dim(d_output, slab_start, TOK_DEV, 0).astype(jnp.float32)
            query_nope = query_slab[..., :nope_width]
            query_rope = query_slab[..., nope_width:]
            scores = (jnp.einsum('ihd,jhd->hij', query_nope, key_nope) + jnp.einsum('ihr,jr->hij', query_rope, key_rope)) * score_scale
            probs = jax.nn.softmax(scores, axis=-1)
            probs_low = probs.astype(jnp.bfloat16).astype(jnp.float32)
            attended = jnp.einsum('hij,jhd->ihd', probs_low, values_here)
            row_delta = lax.optimization_barrier(jnp.sum(output_grad * attended, axis=-1))
            grad_probs = jnp.einsum('ihd,jhd->hij', output_grad, values_here)
            score_grads = probs * (grad_probs - jnp.transpose(row_delta)[:, :, None])
            score_low = score_grads.astype(jnp.bfloat16).astype(jnp.float32)
            grad_nope = jnp.einsum('hij,jhd->ihd', score_low, key_nope)
            grad_rope = jnp.einsum('hij,jr->ihr', score_low, key_rope)
            query_grads.append(jnp.concatenate([grad_nope, grad_rope], axis=-1) * score_scale)
            key_grad = (jnp.einsum('hij,ihd->jhd', score_low, query_nope) * score_scale).astype(jnp.bfloat16)
            value_grad = jnp.einsum('hij,ihd->jhd', probs_low, output_grad).astype(jnp.bfloat16)
            key_total = key_total + key_grad.astype(jnp.float32)
            value_total = value_total + value_grad.astype(jnp.float32)
            rope_total = rope_total + jnp.einsum('hij,ihr->jr', score_low, query_rope) * score_scale
        latent_wide = latent.astype(jnp.float32)
        latent_grad = jnp.einsum('jhd,chd->jc', key_total, uk_wide) + jnp.einsum('jhd,chd->jc', value_total, uv_wide)
        grad_uk = grad_uk + jnp.einsum('jc,jhd->chd', latent_wide, key_total)
        grad_uv = grad_uv + jnp.einsum('jc,jhd->chd', latent_wide, value_total)
        row_grads = jnp.concatenate([latent_grad, rope_total], axis=1)
        return ((grad_uk, grad_uv), (jnp.concatenate(query_grads, axis=0), row_grads))
    start_totals = (jnp.zeros((LATENT, HEADS, NOPE_DIM), jnp.float32), jnp.zeros((LATENT, HEADS, VALUE_DIM), jnp.float32))
    sequences = jnp.arange(TOKENS // span_rows, dtype=jnp.int32)
    final_totals, stacked = lax.scan(one_sequence, start_totals, sequences)
    query_out = stacked[0].reshape(TOKENS, HEADS, NOPE_DIM + ROPE_DIM)
    rows_out = stacked[1].reshape(TOKENS, LATENT + ROPE_DIM)
    return (query_out, rows_out, final_totals[0], final_totals[1])
```

```python
import functools
import math

import jax
import jax.numpy as jnp
from jax import lax
from jax.experimental import pallas as pl
from jax.experimental.pallas import tpu as pltpu
from jax.sharding import PartitionSpec as P


GROUP = 4
CHUNK_HEADS = 16
BF = jnp.bfloat16
F32 = jnp.float32


def flip_send(value, axis, mask):
    return lax.ppermute(value, axis, [(i, i ^ mask) for i in range(lax.axis_size(axis))])


def dot(a, b, ca, cb):
    return lax.dot_general(a, b, (((ca,), (cb,)), ((), ())), preferred_element_type=F32)


def by_head(block_ref, wide_ref, put):
    rows, heads, width = block_ref.shape
    lanes = wide_ref.shape[1]
    for at in range(0, width, lanes):
        n = min(lanes, width - at)
        piece = block_ref[:, :, at : at + n].astype(F32).reshape(rows * heads, n)
        wide_ref[: rows * heads, :n] = piece
        for h in range(heads):
            put(h, slice(at, at + n), wide_ref[pl.ds(h, rows, heads), :][:, :n].astype(BF))


def pair_kernel(first, width, nope, orders, scale, *refs):
    pos_ref, slots_ref, lat_t_ref, q_block, do_block, uk_block, uv_block = refs[:7]
    refs = refs[7:]
    if not first:
        lg_in, rg_in, _ = refs[:3]
        refs = refs[3:]
    lg_ref, rg_ref, dq_ref, keep_a_ref, send_a_ref, keep_b_ref, send_b_ref = refs[:7]
    lat_a_ref, lat_b_ref, w_ref, q_ref, do_ref, deep_ref = refs[7:]
    step = pl.program_id(0)
    per_block = dq_ref.shape[1] // 2
    at = step % per_block

    @pl.when(at == 0)
    def _():
        def put_q(h, lanes, x):
            q_ref[h, :, lanes] = x

        def put_do(h, lanes, x):
            do_ref[h, :, lanes] = x

        def put_uk(h, lanes, x):
            w_ref[h // 2, :, (h % 2) * nope : (h % 2 + 1) * nope] = x

        def put_uv(h, lanes, x):
            w_ref[h // 2, :, (2 + h % 2) * nope : (3 + h % 2) * nope] = x

        by_head(q_block, deep_ref, put_q)
        by_head(do_block, deep_ref, put_do)
        by_head(uk_block, deep_ref, put_uk)
        by_head(uv_block, deep_ref, put_uv)

    @pl.when(step == 0)
    def _():
        if first:
            lg_ref[...] = jnp.zeros_like(lg_ref)
            rg_ref[...] = jnp.zeros_like(rg_ref)
        else:
            lg_ref[...] = lg_in[...]
            rg_ref[...] = rg_in[...]
        position = pos_ref[0]
        for order, lat_ref in zip(orders, (lat_a_ref, lat_b_ref)):
            blocks = 1 << len(order)
            each = width // blocks
            for t in range(blocks):
                k = sum(((t >> (len(order) - 1 - n)) & 1) << bit for n, bit in enumerate(order))
                row = pl.multiple_of((position ^ k) * each, each)
                lat_ref[t * each : (t + 1) * each] = lat_t_ref[pl.ds(row, each), :]

    ukv = w_ref[at]
    kv = dot(slots_ref[:, :width], ukv, 1, 0).astype(BF)
    key_rope = slots_ref[:, width:]
    kcs, ss, gps = [], [], []
    for e in range(2):
        kcs.append(jnp.concatenate([kv[:, e * nope : (e + 1) * nope], key_rope], axis=1))
        ss.append(dot(kcs[e], q_ref[2 * at + e], 1, 1))
        gps.append(dot(kv[:, (2 + e) * nope : (3 + e) * nope], do_ref[2 * at + e], 1, 1))
    lows, dss = [], []
    for e in range(2):
        p = jnp.exp((ss[e] - jnp.max(ss[e], axis=0, keepdims=True)) * scale)
        p = p * (1.0 / jnp.sum(p, axis=0, keepdims=True))
        lows.append(p.astype(BF))
        delta = jnp.sum(lows[e].astype(F32) * gps[e], axis=0, keepdims=True)
        dss.append((p * (gps[e] - delta)).astype(BF))
    dks, dvs, dqs = [], [], []
    for e in range(2):
        dkc = dot(dss[e], q_ref[2 * at + e], 1, 0) * scale
        dvs.append(dot(lows[e], do_ref[2 * at + e], 1, 0).astype(BF))
        dks.append(dkc[:, :nope].astype(BF))
        rg_ref[...] += dkc[:, nope:]
        dqs.append(dot(dss[e], kcs[e], 0, 0) * scale)
    grads = jnp.concatenate(dks + dvs, axis=1)
    lg_ref[...] += dot(grads, ukv, 1, 1)
    half = keep_a_ref.shape[0]
    for at_w, (lat_ref, keep_ref, send_ref) in enumerate(
        ((lat_a_ref, keep_a_ref, send_a_ref), (lat_b_ref, keep_b_ref, send_b_ref))
    ):
        grad = grads[:, at_w * 2 * nope : (at_w + 1) * 2 * nope]
        dw = dot(lat_ref[...], grad, 1, 0).astype(BF)
        keep_ref[...] = dw[:half]
        send_ref[...] = dw[half:]
    for q in range(per_block):

        @pl.when(at == q)
        def _(q=q):
            for e in range(2):
                dq_ref[:, 2 * q + e, :] = dqs[e]


def chunk_sizes(heads):
    sizes = []
    left = heads
    while left > CHUNK_HEADS:
        sizes.append(CHUNK_HEADS)
        left -= CHUNK_HEADS
    if left % 16 == 0:
        return sizes + [left // 2, left // 2]
    return sizes + [left]


def per_device(compressed, query, d_output, w_uk, w_uv):
    rows = compressed.shape[0]
    width = w_uk.shape[0]
    heads = w_uk.shape[1]
    nope = w_uk.shape[2]
    rope = query.shape[2] - nope
    scale = 1.0 / math.sqrt(query.shape[2])
    ctx = lax.axis_size("ctx")
    bits = ctx.bit_length() - 1
    group_bits = GROUP.bit_length() - 1
    position = lax.axis_index("ctx")
    span = rows * GROUP
    slots = jnp.concatenate(
        [compressed] + [flip_send(compressed, "ctx", m) for m in range(1, GROUP)], axis=0
    )
    lat_t = jnp.transpose(slots[:, :width])
    rows_each = width // ctx
    far = list(range(group_bits, bits))
    orders = [[0, 1] + far, [1, 0] + far]
    params = pltpu.CompilerParams(
        dimension_semantics=("arbitrary",), vmem_limit_bytes=56 * 1024 * 1024
    )
    lg = rg = dq = None
    flows = []
    start = 0
    for c, chunk in enumerate(chunk_sizes(heads)):
        dq_heads = min(8, chunk)
        per_dq = dq_heads // 2
        first = c == 0
        whole = lambda shape: pl.BlockSpec(shape, lambda g: (0,) * len(shape))
        offset = start // dq_heads
        head_block = lambda n, w, offset=offset, per_dq=per_dq, dq_heads=dq_heads: pl.BlockSpec(
            (n, dq_heads, w), lambda g: (0, offset + g // per_dq, 0)
        )
        by_lane = lambda n, w: pl.BlockSpec((n, w), lambda g: (0, g))
        ins = [position.astype(jnp.int32).reshape(1), slots, lat_t, query, d_output, w_uk, w_uv]
        in_specs = [
            pl.BlockSpec(memory_space=pltpu.SMEM),
            whole((span, width + rope)),
            whole((width, span)),
            head_block(rows, nope + rope),
            head_block(rows, nope),
            head_block(width, nope),
            head_block(width, nope),
        ]
        alias = {}
        if not first:
            ins += [lg, rg, dq]
            in_specs += [
                whole((span, width)),
                whole((span, rope)),
                pl.BlockSpec(memory_space=pl.ANY),
            ]
            alias = {9: 2}
        half_spec = by_lane(width // 2, 2 * nope)
        half_shape = jax.ShapeDtypeStruct((width // 2, chunk * nope), BF)
        lg, rg, dq, keep_a, send_a, keep_b, send_b = pl.pallas_call(
            functools.partial(pair_kernel, first, width, nope, orders, scale),
            grid=(chunk // 2,),
            in_specs=in_specs,
            out_specs=[
                whole((span, width)),
                whole((span, rope)),
                head_block(rows, nope + rope),
                half_spec,
                half_spec,
                half_spec,
                half_spec,
            ],
            out_shape=[
                jax.ShapeDtypeStruct((span, width), F32),
                jax.ShapeDtypeStruct((span, rope), F32),
                jax.ShapeDtypeStruct((rows, heads, nope + rope), F32),
                half_shape,
                half_shape,
                half_shape,
                half_shape,
            ],
            scratch_shapes=[
                pltpu.VMEM((width, span), BF),
                pltpu.VMEM((width, span), BF),
                pltpu.VMEM((per_dq, width, 4 * nope), BF),
                pltpu.VMEM((dq_heads, rows, nope + rope), BF),
                pltpu.VMEM((dq_heads, rows, nope), BF),
                pltpu.VMEM((dq_heads * max(rows, width), nope), F32),
            ],
            input_output_aliases=alias,
            compiler_params=params,
        )(*ins)
        flows.append([(keep_a, send_a), (keep_b, send_b)])
        start += chunk

    grads = []
    for w, order in enumerate(orders):
        finals = []
        for flow in flows:
            keep, send = flow[w]
            for at_bit, bit in enumerate(order):
                came = flip_send(send, "ctx", 1 << bit)
                total = keep.astype(F32) + came.astype(F32)
                if at_bit == bits - 1:
                    finals.append(total)
                else:
                    total = total.astype(BF)
                    half = total.shape[0] // 2
                    keep, send = total[:half], total[half:]
        grads.append(jnp.concatenate(finals, axis=1).reshape(rows_each, heads, nope))

    partial = jnp.concatenate([lg, rg], axis=1)
    for bit in reversed(range(group_bits)):
        half = partial.shape[0] // 2
        partial = partial[:half] + flip_send(partial[half:].astype(BF), "ctx", 1 << bit).astype(F32)
    n_head = lax.axis_size("head")
    own = lax.axis_index("head")
    piece = rows // n_head
    cut = lambda i: lax.dynamic_slice_in_dim(partial, (i % n_head) * piece, piece, 0)
    d_compressed = cut(own)
    for r in range(1, n_head):
        d_compressed = d_compressed + lax.ppermute(
            cut(own + r), "head", [(i, (i + r) % n_head) for i in range(n_head)]
        )
    return (dq, d_compressed, *grads)


def solution(mesh):
    placed = (
        P("ctx", None),
        P("ctx", "head", None),
        P("ctx", "head", None),
        P(None, "head", None),
        P(None, "head", None),
    )

    return jax.shard_map(
        per_device,
        mesh=mesh,
        in_specs=placed,
        out_specs=(
            P("ctx", "head", None),
            P(("ctx", "head"), None),
            P("ctx", "head", None),
            P("ctx", "head", None),
        ),
        check_vma=False,
    )
```

```python
import functools
import math

import jax
import jax.numpy as jnp
from jax import lax
from jax.experimental import pallas as pl
from jax.experimental.pallas import tpu as pltpu
from jax.sharding import PartitionSpec as P


GROUP = 4
CHUNK_HEADS = 16
BF = jnp.bfloat16
F32 = jnp.float32


def flip_send(value, axis, mask):
    return lax.ppermute(value, axis, [(i, i ^ mask) for i in range(lax.axis_size(axis))])


def dot(a, b, ca, cb):
    return lax.dot_general(a, b, (((ca,), (cb,)), ((), ())), preferred_element_type=F32)


def by_head(block_ref, wide_ref, put):
    rows, heads, width = block_ref.shape
    deep, lanes = wide_ref.shape
    some = deep // heads

    def move(r, carry):
        row = pl.ds(pl.multiple_of(r * some, some), some)
        for at in range(0, width, lanes):
            n = min(lanes, width - at)
            piece = block_ref[row, :, at : at + n].astype(F32).reshape(some * heads, n)
            wide_ref[:, :n] = piece
            for h in range(heads):
                part = wide_ref[pl.ds(h, some, heads), :][:, :n].astype(BF)
                put(h, row, slice(at, at + n), part)
        return carry

    lax.fori_loop(0, rows // some, move, 0)


def pair_kernel(first, width, nope, orders, scale, *refs):
    pos_ref, slots_ref, lat_t_ref, q_block, do_block, uk_block, uv_block = refs[:7]
    refs = refs[7:]
    if not first:
        lg_in, rg_in, _ = refs[:3]
        refs = refs[3:]
    lg_ref, rg_ref, dq_ref, keep_a_ref, send_a_ref, keep_b_ref, send_b_ref = refs[:7]
    lat_a_ref, lat_b_ref, w_ref, q_ref, do_ref, deep_ref, dq_near_ref, dq_far_ref = refs[7:]
    step = pl.program_id(0)
    per_block = dq_ref.shape[1] // 2
    at = step % per_block

    @pl.when(at == 0)
    def _():
        def put_q(h, row, lanes, x):
            q_ref[h, row, lanes] = x

        def put_do(h, row, lanes, x):
            do_ref[h, row, lanes] = x

        def put_uk(h, row, lanes, x):
            w_ref[h // 2, row, (h % 2) * nope : (h % 2 + 1) * nope] = x

        def put_uv(h, row, lanes, x):
            w_ref[h // 2, row, (2 + h % 2) * nope : (3 + h % 2) * nope] = x

        by_head(q_block, deep_ref, put_q)
        by_head(do_block, deep_ref, put_do)
        by_head(uk_block, deep_ref, put_uk)
        by_head(uv_block, deep_ref, put_uv)

    @pl.when(step == 0)
    def _():
        if first:
            lg_ref[...] = jnp.zeros_like(lg_ref)
            rg_ref[...] = jnp.zeros_like(rg_ref)
        else:
            lg_ref[...] = lg_in[...]
            rg_ref[...] = rg_in[...]
        position = pos_ref[0]
        for order, lat_ref in zip(orders, (lat_a_ref, lat_b_ref)):
            blocks = 1 << len(order)
            each = width // blocks
            for t in range(blocks):
                k = sum(((t >> (len(order) - 1 - n)) & 1) << bit for n, bit in enumerate(order))
                row = pl.multiple_of((position ^ k) * each, each)
                lat_ref[t * each : (t + 1) * each] = lat_t_ref[pl.ds(row, each), :]

    ukv = w_ref[at]
    kv = dot(slots_ref[:, :width], ukv, 1, 0).astype(BF)
    key_rope = slots_ref[:, width:]
    kcs, ss, gps = [], [], []
    for e in range(2):
        kcs.append(jnp.concatenate([kv[:, e * nope : (e + 1) * nope], key_rope], axis=1))
        ss.append(dot(kcs[e], q_ref[2 * at + e], 1, 1))
        gps.append(dot(kv[:, (2 + e) * nope : (3 + e) * nope], do_ref[2 * at + e], 1, 1))
    lows, dss = [], []
    for e in range(2):
        p = jnp.exp((ss[e] - jnp.max(ss[e], axis=0, keepdims=True)) * scale)
        p = p * (1.0 / jnp.sum(p, axis=0, keepdims=True))
        lows.append(p.astype(BF))
        delta = jnp.sum(lows[e].astype(F32) * gps[e], axis=0, keepdims=True)
        dss.append((p * (gps[e] - delta)).astype(BF))
    dks, dvs, dqs = [], [], []
    for e in range(2):
        dkc = dot(dss[e], q_ref[2 * at + e], 1, 0) * scale
        dvs.append(dot(lows[e], do_ref[2 * at + e], 1, 0).astype(BF))
        dks.append(dkc[:, :nope].astype(BF))
        rg_ref[...] += dkc[:, nope:]
        dqs.append(dot(dss[e], kcs[e], 0, 0) * scale)
    grads = jnp.concatenate(dks + dvs, axis=1)
    lg_ref[...] += dot(grads, ukv, 1, 1)
    half = keep_a_ref.shape[0]
    for at_w, (lat_ref, keep_ref, send_ref) in enumerate(
        ((lat_a_ref, keep_a_ref, send_a_ref), (lat_b_ref, keep_b_ref, send_b_ref))
    ):
        grad = grads[:, at_w * 2 * nope : (at_w + 1) * 2 * nope]
        dw = dot(lat_ref[...], grad, 1, 0).astype(BF)
        keep_ref[...] = dw[:half]
        send_ref[...] = dw[half:]
    rows, block_heads, deep = dq_ref.shape
    for e in range(2):
        spot = pl.ds(2 * at + e, rows, block_heads)
        dq_near_ref[spot, :] = dqs[e][:, :nope]
        dq_far_ref[spot, :] = jnp.concatenate(
            [dqs[e][:, nope:], jnp.zeros((rows, 2 * nope - deep), F32)], axis=1
        )

    @pl.when(at == per_block - 1)
    def _():
        dq_ref[:, :, :nope] = dq_near_ref[...].reshape(rows, block_heads, nope)
        dq_ref[:, :, nope:] = dq_far_ref[...].reshape(rows, block_heads, nope)[:, :, : deep - nope]


def chunk_sizes(heads):
    sizes = []
    left = heads
    while left > CHUNK_HEADS:
        sizes.append(CHUNK_HEADS)
        left -= CHUNK_HEADS
    if left % 16 == 0:
        return sizes + [left // 2, left // 2]
    return sizes + [left]


def per_device(compressed, query, d_output, w_uk, w_uv):
    rows = compressed.shape[0]
    width = w_uk.shape[0]
    heads = w_uk.shape[1]
    nope = w_uk.shape[2]
    rope = query.shape[2] - nope
    scale = 1.0 / math.sqrt(query.shape[2])
    ctx = lax.axis_size("ctx")
    bits = ctx.bit_length() - 1
    group_bits = GROUP.bit_length() - 1
    position = lax.axis_index("ctx")
    span = rows * GROUP
    slots = jnp.concatenate(
        [compressed] + [flip_send(compressed, "ctx", m) for m in range(1, GROUP)], axis=0
    )
    lat_t = jnp.transpose(slots[:, :width])
    rows_each = width // ctx
    far = list(range(group_bits, bits))
    orders = [[0, 1] + far, [1, 0] + far]
    params = pltpu.CompilerParams(
        dimension_semantics=("arbitrary",), vmem_limit_bytes=56 * 1024 * 1024
    )
    lg = rg = dq = None
    flows = []
    start = 0
    for c, chunk in enumerate(chunk_sizes(heads)):
        dq_heads = min(8, chunk)
        per_dq = dq_heads // 2
        first = c == 0
        whole = lambda shape: pl.BlockSpec(shape, lambda g: (0,) * len(shape))
        offset = start // dq_heads
        head_block = lambda n, w, offset=offset, per_dq=per_dq, dq_heads=dq_heads: pl.BlockSpec(
            (n, dq_heads, w), lambda g: (0, offset + g // per_dq, 0)
        )
        by_lane = lambda n, w: pl.BlockSpec((n, w), lambda g: (0, g))
        ins = [position.astype(jnp.int32).reshape(1), slots, lat_t, query, d_output, w_uk, w_uv]
        in_specs = [
            pl.BlockSpec(memory_space=pltpu.SMEM),
            whole((span, width + rope)),
            whole((width, span)),
            head_block(rows, nope + rope),
            head_block(rows, nope),
            head_block(width, nope),
            head_block(width, nope),
        ]
        alias = {}
        if not first:
            ins += [lg, rg, dq]
            in_specs += [
                whole((span, width)),
                whole((span, rope)),
                pl.BlockSpec(memory_space=pl.ANY),
            ]
            alias = {9: 2}
        half_spec = by_lane(width // 2, 2 * nope)
        half_shape = jax.ShapeDtypeStruct((width // 2, chunk * nope), BF)
        lg, rg, dq, keep_a, send_a, keep_b, send_b = pl.pallas_call(
            functools.partial(pair_kernel, first, width, nope, orders, scale),
            grid=(chunk // 2,),
            in_specs=in_specs,
            out_specs=[
                whole((span, width)),
                whole((span, rope)),
                head_block(rows, nope + rope),
                half_spec,
                half_spec,
                half_spec,
                half_spec,
            ],
            out_shape=[
                jax.ShapeDtypeStruct((span, width), F32),
                jax.ShapeDtypeStruct((span, rope), F32),
                jax.ShapeDtypeStruct((rows, heads, nope + rope), F32),
                half_shape,
                half_shape,
                half_shape,
                half_shape,
            ],
            scratch_shapes=[
                pltpu.VMEM((width, span), BF),
                pltpu.VMEM((width, span), BF),
                pltpu.VMEM((per_dq, width, 4 * nope), BF),
                pltpu.VMEM((dq_heads, rows, nope + rope), BF),
                pltpu.VMEM((dq_heads, rows, nope), BF),
                pltpu.VMEM((dq_heads * math.gcd(rows, width), nope), F32),
                pltpu.VMEM((dq_heads * rows, nope), F32),
                pltpu.VMEM((dq_heads * rows, nope), F32),
            ],
            input_output_aliases=alias,
            compiler_params=params,
        )(*ins)
        flows.append([(keep_a, send_a), (keep_b, send_b)])
        start += chunk

    grads = []
    for w, order in enumerate(orders):
        finals = []
        for flow in flows:
            keep, send = flow[w]
            for at_bit, bit in enumerate(order):
                came = flip_send(send, "ctx", 1 << bit)
                total = keep.astype(F32) + came.astype(F32)
                if at_bit == bits - 1:
                    finals.append(total)
                else:
                    total = total.astype(BF)
                    half = total.shape[0] // 2
                    keep, send = total[:half], total[half:]
        grads.append(jnp.concatenate(finals, axis=1).reshape(rows_each, heads, nope))

    partial = jnp.concatenate([lg, rg], axis=1)
    for bit in reversed(range(group_bits)):
        half = partial.shape[0] // 2
        partial = partial[:half] + flip_send(partial[half:].astype(BF), "ctx", 1 << bit).astype(F32)
    n_head = lax.axis_size("head")
    own = lax.axis_index("head")
    piece = rows // n_head
    cut = lambda i: lax.dynamic_slice_in_dim(partial, (i % n_head) * piece, piece, 0)
    d_compressed = cut(own)
    for r in range(1, n_head):
        d_compressed = d_compressed + lax.ppermute(
            cut(own + r), "head", [(i, (i + r) % n_head) for i in range(n_head)]
        )
    return (dq, d_compressed, *grads)


def solution(mesh):
    placed = (
        P("ctx", None),
        P("ctx", "head", None),
        P("ctx", "head", None),
        P(None, "head", None),
        P(None, "head", None),
    )

    return jax.shard_map(
        per_device,
        mesh=mesh,
        in_specs=placed,
        out_specs=(
            P("ctx", "head", None),
            P(("ctx", "head"), None),
            P("ctx", "head", None),
            P("ctx", "head", None),
        ),
        check_vma=False,
    )
```
